32 devices in a mesh: dp: 4 (over x, y), sp: 8 (over z, core).
Axes of the slice: x: 2, y: 2, z: 4, core: 2. Of those that a mesh axis runs over, the one named last changes fastest.
Arguments:
- x: bfloat16 [16384, 2048], P(('dp', 'sp')), parts along dimension 0
- gain: bfloat16 [2048], replicated
- wq: bfloat16 [2048, 4096], replicated
- wk: bfloat16 [2048, 2048], replicated
- wv: bfloat16 [2048, 2048], replicated
- wo: bfloat16 [4096, 2048], replicated
Outputs:
- output: bfloat16 [16384, 2048], P(('dp', 'sp')), parts along dimension 0
There are 4 independent parts. The reference program is written for one: setup_inputs(seed, part) draws one part's arguments, and reference() takes and returns one part's arrays. A program takes and returns all parts, laid end to end along the dimension named above; an argument that names none is the same for every part.
All inputs are finite; a program needn't handle non-finite values.
Results may differ from the reference program's by a relative error of at most 0.012.
Values are sent between devices in bfloat16 or wider.
A program may use at most 2 GiB of HBM per device.

```python
import jax
import jax.numpy as jnp
from jax import lax

ROWS = 4096
D = 2048
HEADS = 32
KV_HEADS = 16
HEAD = 128
THETA = 10000


def setup_inputs(seed: int = 0, part: int = 0) -> dict:
    kx, kn, kq, kk, kv, ko = jax.random.split(jax.random.key(seed), 6)

    def weights(key, rows, columns):
        return jax.random.normal(key, (rows, columns), jnp.float32) * rows**-0.5

    drawn = {
        "x": jax.random.normal(jax.random.fold_in(kx, part), (ROWS, D), jnp.float32),
        "gain": 1 + 0.1 * jax.random.normal(kn, (D,), jnp.float32),
        "wq": 2 * weights(kq, D, HEADS * HEAD),
        "wk": 2 * weights(kk, D, KV_HEADS * HEAD),
        "wv": 4 * weights(kv, D, KV_HEADS * HEAD),
        "wo": weights(ko, HEADS * HEAD, D),
    }
    return {k: v.astype(jnp.bfloat16) for k, v in drawn.items()}


def normed(x, gain):
    wide = x.astype(jnp.float32)
    scale = lax.rsqrt(jnp.mean(wide * wide, -1, keepdims=True) + 1e-6)
    return (wide * scale * gain.astype(jnp.float32)).astype(jnp.bfloat16)


def turned(t, place, theta):
    half = t.shape[-1] // 2
    angle = place.astype(jnp.float32)[:, None] * theta ** (-jnp.arange(half, dtype=jnp.float32) / half)
    cos, sin = jnp.cos(angle)[:, None], jnp.sin(angle)[:, None]
    a, b = t[..., :half].astype(jnp.float32), t[..., half:].astype(jnp.float32)
    return jnp.concatenate([a * cos - b * sin, b * cos + a * sin], -1).astype(jnp.bfloat16)


def matmul(a, w):
    return jnp.dot(a, w, preferred_element_type=jnp.float32).astype(jnp.bfloat16)


def einsum(form, a, b):
    return jnp.einsum(form, a.astype(jnp.float32), b.astype(jnp.float32))


def attention(q, k, v):
    scores = einsum("tgsd,ugd->gstu", q, k) * q.shape[-1] ** -0.5
    token = jnp.arange(q.shape[0])
    scores = jnp.where(token[:, None] >= token, scores, -jnp.inf)
    weights = jax.nn.softmax(scores, -1).astype(jnp.bfloat16)
    return einsum("gstu,ugd->tgsd", weights, v).astype(jnp.bfloat16)


def reference(x, gain, wq, wk, wv, wo):
    a, place = normed(x, gain), jnp.arange(ROWS)
    q = turned(matmul(a, wq).reshape(ROWS, HEADS, HEAD), place, THETA).reshape(ROWS, KV_HEADS, -1, HEAD)
    k = turned(matmul(a, wk).reshape(ROWS, KV_HEADS, HEAD), place, THETA)
    v = matmul(a, wv).reshape(ROWS, KV_HEADS, HEAD)
    seen = attention(q, k, v).reshape(ROWS, HEADS * HEAD)
    return (x.astype(jnp.float32) + jnp.dot(seen, wo, preferred_element_type=jnp.float32)).astype(jnp.bfloat16)
```

```python
import functools

import jax
import jax.numpy as jnp
from jax import lax
from jax.experimental import pallas as pl
from jax.experimental.pallas import tpu as pltpu
from jax.sharding import PartitionSpec as P

HEAD = 128
THETA = 10000
NEG = -1e30
HIDDEN = 2 * NEG
LOG2E = 1.4426950408889634
VMEM = 60 * 2**20
ONES = 8
PIECES = (128, 128, 128, 128)
BQ = 256
BK = 256


def _dot(a, b, ca, cb):
    return lax.dot_general(a, b, (((ca,), (cb,)), ((), ())), preferred_element_type=jnp.float32)


def normed(x, gain):
    wide = x.astype(jnp.float32)
    scale = lax.rsqrt(jnp.mean(wide * wide, -1, keepdims=True) + 1e-6)
    return (wide * scale * gain.astype(jnp.float32)).astype(jnp.bfloat16)


def tables(place):
    half = HEAD // 2
    angle = place.astype(jnp.float32)[:, None] * THETA ** (-jnp.arange(half, dtype=jnp.float32) / half)
    cos, sin = jnp.cos(angle), jnp.sin(angle)
    return jnp.concatenate([cos, cos], 1), jnp.concatenate([-sin, sin], 1)


def _turn(t, cos, sin):
    t = t.astype(jnp.bfloat16).astype(jnp.float32)
    return (t * cos + pltpu.roll(t, HEAD // 2, 1) * sin).astype(jnp.bfloat16)


def _heads(ref, rows, t, cos, sin):
    for h in range(t.shape[1] // HEAD):
        ref[h, rows, :] = _turn(t[:, h * HEAD : (h + 1) * HEAD], cos, sin)


def _values(ref, rows, t):
    n = t.shape[0]
    for h in range(t.shape[1] // HEAD):
        ref[h, :HEAD, rows] = t[:, h * HEAD : (h + 1) * HEAD].astype(jnp.bfloat16).T
        ref[h, HEAD:, rows] = jnp.ones((ONES, n), jnp.bfloat16)


def _project_own(core_ref, own_ref, pair_ref, wq_ref, wk_ref, wv_ref, cos_ref, sin_ref, q_ref, k_ref, v_ref):
    rows = own_ref.shape[0]
    for n, a_ref in enumerate((own_ref, pair_ref)):
        a = a_ref[...]
        at = pl.multiple_of((core_ref[0] if n == 0 else 1 - core_ref[0]) * rows, rows)
        here = pl.ds(at, rows)
        cos, sin = cos_ref[here, :], sin_ref[here, :]
        _heads(q_ref, here, _dot(a, wq_ref[...], 1, 0), cos, sin)
        _heads(k_ref, here, _dot(a, wk_ref[...], 1, 0), cos, sin)
        _values(v_ref, here, _dot(a, wv_ref[...], 1, 0))


def project_own(core, own, pair, wq, wk, wv, cos, sin):
    rows, depth = own.shape
    kv = wk.shape[1] // HEAD // 2
    steps = 4
    cols = kv * HEAD // steps
    whole = lambda j, c: (0, 0)
    part = lambda j, c: (0, c[0] * steps + j)
    head = lambda j, c: (j, 0, 0)
    return pl.pallas_call(
        _project_own,
        grid_spec=pltpu.PrefetchScalarGridSpec(
            num_scalar_prefetch=1,
            grid=(steps,),
            in_specs=[pl.BlockSpec((rows, depth), whole)] * 2
            + [pl.BlockSpec((depth, 2 * cols), part), pl.BlockSpec((depth, cols), part), pl.BlockSpec((depth, cols), part)]
            + [pl.BlockSpec((2 * rows, HEAD), whole)] * 2,
            out_specs=[
                pl.BlockSpec((2 * kv // steps, 2 * rows, HEAD), head),
                pl.BlockSpec((kv // steps, 2 * rows, HEAD), head),
                pl.BlockSpec((kv // steps, HEAD + ONES, 2 * rows), head),
            ],
        ),
        out_shape=[
            jax.ShapeDtypeStruct((2 * kv, 2 * rows, HEAD), jnp.bfloat16),
            jax.ShapeDtypeStruct((kv, 2 * rows, HEAD), jnp.bfloat16),
            jax.ShapeDtypeStruct((kv, HEAD + ONES, 2 * rows), jnp.bfloat16),
        ],
        compiler_params=pltpu.CompilerParams(dimension_semantics=("arbitrary",), vmem_limit_bytes=VMEM),
        cost_estimate=pl.CostEstimate(flops=4 * rows * depth * 4 * kv * HEAD, transcendentals=0, bytes_accessed=8 * depth * kv * HEAD),
        name="project_own",
    )(core, own, pair, wq, wk, wv, cos, sin)


def _project_kv(core_ref, a_ref, wk_ref, wv_ref, cos_ref, sin_ref, k_ref, v_ref):
    a = a_ref[...]
    rows = slice(None)
    _heads(k_ref, rows, _dot(a, wk_ref[...], 1, 0), cos_ref[...], sin_ref[...])
    _values(v_ref, rows, _dot(a, wv_ref[...], 1, 0))


def project_kv(core, a, wk, wv, cos, sin):
    rows, depth = a.shape
    kv = wk.shape[1] // HEAD // 2
    steps = 4
    cols = kv * HEAD // steps
    whole = lambda j, c: (0, 0)
    part = lambda j, c: (0, c[0] * steps + j)
    head = lambda j, c: (j, 0, 0)
    return pl.pallas_call(
        _project_kv,
        grid_spec=pltpu.PrefetchScalarGridSpec(
            num_scalar_prefetch=1,
            grid=(steps,),
            in_specs=[pl.BlockSpec((rows, depth), whole), pl.BlockSpec((depth, cols), part), pl.BlockSpec((depth, cols), part)]
            + [pl.BlockSpec((rows, HEAD), whole)] * 2,
            out_specs=[pl.BlockSpec((kv // steps, rows, HEAD), head), pl.BlockSpec((kv // steps, HEAD + ONES, rows), head)],
        ),
        out_shape=[
            jax.ShapeDtypeStruct((kv, rows, HEAD), jnp.bfloat16),
            jax.ShapeDtypeStruct((kv, HEAD + ONES, rows), jnp.bfloat16),
        ],
        compiler_params=pltpu.CompilerParams(dimension_semantics=("arbitrary",), vmem_limit_bytes=VMEM),
        cost_estimate=pl.CostEstimate(flops=2 * rows * depth * 2 * kv * HEAD, transcendentals=0, bytes_accessed=4 * depth * kv * HEAD),
        name="project_kv",
    )(core, a, wk, wv, cos, sin)


def _attend(count_ref, q_ref, k_ref, v_ref, *rest, causal, scale, bk, carried, last):
    rest = list(rest)
    top_in, mix_in = (rest.pop(0), rest.pop(0)) if carried else (None, None)
    if last:
        o_ref, top, mix = rest[:3]
        rest = rest[3:]
    else:
        top, mix = rest[:2]
        rest = rest[2:]
    kb, g, bq, d = q_ref.shape
    cols = g * bq
    iq = pl.program_id(0)
    e = scale * LOG2E
    if carried:
        top[...] = top_in[...]
        mix[...] = mix_in[...]
    else:
        top[...] = jnp.full(top.shape, NEG, jnp.float32)
        mix[...] = jnp.zeros(mix.shape, jnp.float32)
    if causal:
        gap = lax.rem(lax.broadcasted_iota(jnp.int32, (bk, cols), 1), bq) - lax.broadcasted_iota(jnp.int32, (bk, cols), 0)
        rest[0][...] = gap

    def block(j, masked):
        here = pl.ds(pl.multiple_of(j * bk, bk), bk)
        scores = [_dot(k_ref[i, here, :], q_ref[i].reshape(cols, d), 1, 1) for i in range(kb)]
        if masked:
            ok = rest[0][...] >= j * bk - iq * bq
        weights, keeps = [], []
        for i, s in enumerate(scores):
            if masked:
                s = jnp.where(ok, s, HIDDEN)
            old = top[0, i : i + 1, :]
            new = jnp.maximum(old, s.max(axis=0, keepdims=True))
            top[0, i : i + 1, :] = new
            weights.append(jnp.exp2((s - new) * e).astype(jnp.bfloat16))
            keeps.append(jnp.exp2((old - new) * e))
        for i, (p, keep) in enumerate(zip(weights, keeps)):
            mix[0, i] = mix[0, i] * keep + _dot(v_ref[i, :, here], p, 1, 0)

    whole = lax.div(iq * bq, bk) if causal else count_ref[0]
    lax.fori_loop(0, whole, lambda j, _: block(j, False), None)
    if causal:
        lax.fori_loop(whole, lax.div(iq * bq + bq + bk - 1, bk), lambda j, _: block(j, True), None)
    if last:
        for i in range(kb):
            out = mix[0, i, :HEAD, :] * (1 / mix[0, i, HEAD : HEAD + 1, :])
            for n in range(g):
                at = (i * g + n) * HEAD
                o_ref[:, at : at + HEAD] = out[:, n * bq : (n + 1) * bq].T.astype(o_ref.dtype)


def attend(count, q, k, v, state=None, causal=False, last=False):
    heads, sq, d = q.shape
    kv, sk = k.shape[:2]
    g = heads // kv
    nq, cols = sq // BQ, g * BQ
    keys = lambda iq, c: (0, 0, 0)
    specs = [
        pl.BlockSpec((kv, g, BQ, d), lambda iq, c: (0, 0, iq, 0)),
        pl.BlockSpec((kv, sk, d), keys),
        pl.BlockSpec((kv, HEAD + ONES, sk), keys),
    ]
    state_specs = [
        pl.BlockSpec((1, kv, cols), lambda iq, c: (iq, 0, 0)),
        pl.BlockSpec((1, kv, HEAD + ONES, cols), lambda iq, c: (iq, 0, 0, 0)),
    ]
    state_shapes = [jax.ShapeDtypeStruct((nq, kv, cols), jnp.float32), jax.ShapeDtypeStruct((nq, kv, HEAD + ONES, cols), jnp.float32)]
    given = [q.reshape(kv, g, sq, d), k, v]
    scratch = [pltpu.VMEM((BK, cols), jnp.int32)] if causal else []
    aliases = {}
    if state is not None:
        given += list(state)
        specs += state_specs
        if not last:
            aliases = {4: 0, 5: 1}
    if last:
        out_specs = pl.BlockSpec((BQ, heads * d), lambda iq, c: (iq, 0))
        out_shape = jax.ShapeDtypeStruct((sq, heads * d), jnp.bfloat16)
        scratch = [pltpu.VMEM((1, kv, cols), jnp.float32), pltpu.VMEM((1, kv, HEAD + ONES, cols), jnp.float32)] + scratch
    else:
        out_specs, out_shape = state_specs, state_shapes
    return pl.pallas_call(
        functools.partial(_attend, causal=causal, scale=d**-0.5, bk=BK, carried=state is not None, last=last),
        grid_spec=pltpu.PrefetchScalarGridSpec(
            num_scalar_prefetch=1, grid=(nq,), in_specs=specs, out_specs=out_specs, scratch_shapes=scratch,
        ),
        out_shape=out_shape,
        input_output_aliases=aliases,
        compiler_params=pltpu.CompilerParams(dimension_semantics=("arbitrary",), vmem_limit_bytes=VMEM),
        cost_estimate=pl.CostEstimate(flops=4 * heads * sq * sk * d, transcendentals=heads * sq * sk, bytes_accessed=2 * (q.size + k.size + v.size)),
        name="attend_own" if causal else "attend_before",
    )(count, *given)


def _output(half_ref, o_ref, w_ref, add_ref, y_ref):
    y_ref[...] = (_dot(o_ref[...], w_ref[...], 1, 0) + add_ref[...].astype(jnp.float32)).astype(y_ref.dtype)


def output(half, o, wo, add, dtype):
    rows, depth = o.shape
    width = wo.shape[1]
    cols = 512
    column = lambda j, c: (0, j)
    return pl.pallas_call(
        _output,
        grid_spec=pltpu.PrefetchScalarGridSpec(
            num_scalar_prefetch=1,
            grid=(width // cols,),
            in_specs=[
                pl.BlockSpec((rows, depth), lambda j, c: (0, 0)),
                pl.BlockSpec((depth, cols), lambda j, c: (c[0], j)),
                pl.BlockSpec((rows, cols), column),
            ],
            out_specs=pl.BlockSpec((rows, cols), column),
        ),
        out_shape=jax.ShapeDtypeStruct((rows, width), dtype),
        compiler_params=pltpu.CompilerParams(dimension_semantics=("arbitrary",), vmem_limit_bytes=VMEM),
        cost_estimate=pl.CostEstimate(flops=2 * rows * depth * width, transcendentals=0, bytes_accessed=2 * depth * width),
        name="output",
    )(half, o, wo, add)


def solution(mesh):
    devices = mesh.shape["sp"]
    swap = [(d, d ^ 1) for d in range(devices)]

    def step(x, gain, wq, wk, wv, wo):
        rows = x.shape[0]
        me = lax.axis_index("sp")
        chip, core = me // 2, me % 2
        core_s = core.astype(jnp.int32)[None]
        pair_x = lax.ppermute(x, "sp", swap)
        own = normed(x, gain)
        gathered, start = [], 0
        for n in PIECES:
            gathered.append((start, n, lax.all_gather(lax.slice_in_dim(own, start, start + n), "sp", axis=0)))
            start += n
        pair = normed(pair_x, gain)
        cos, sin = tables(chip * 2 * rows + jnp.arange(2 * rows))
        q, k, v = project_own(core_s, own, pair, wq, wk, wv, cos, sin)
        state = attend(core_s, q, k, v, causal=True)
        for i, (start, n, a) in enumerate(gathered):
            place = (jnp.arange(devices - 2)[:, None] * rows + start + jnp.arange(n)).reshape(-1)
            cos, sin = tables(place)
            k, v = project_kv(core_s, a[: devices - 2].reshape(-1, a.shape[-1]), wk, wv, cos, sin)
            count = (chip * 2 * n // BK).astype(jnp.int32)[None]
            state = attend(count, q, k, v, state, last=i == len(PIECES) - 1)
        o = state
        mine = lax.dynamic_slice_in_dim(o, core * rows, rows)
        theirs = lax.dynamic_slice_in_dim(o, (1 - core) * rows, rows)
        theirs = lax.ppermute(theirs, "sp", swap)
        y = output(core_s, mine, wo, x, jnp.float32)
        return output(1 - core_s, theirs, wo, y, jnp.bfloat16)

    tokens, whole = P(("dp", "sp"), None), P(None, None)
    return jax.shard_map(
        step,
        mesh=mesh,
        in_specs=(tokens, P(None), whole, whole, whole, whole),
        out_specs=tokens,
        check_vma=False,
    )
```

```python
import functools

import jax
import jax.numpy as jnp
from jax import lax
from jax.experimental import pallas as pl
from jax.experimental.pallas import tpu as pltpu
from jax.sharding import PartitionSpec as P

HEAD = 128
THETA = 10000
NEG = -1e30
HIDDEN = 2 * NEG
LOG2E = 1.4426950408889634
VMEM = 63 * 2**20
ONES = 8
PIECE = 128
BQ = 256
BK = 256
AHEAD = 2
TILE = 256


def _dot(a, b, ca, cb):
    return lax.dot_general(a, b, (((ca,), (cb,)), ((), ())), preferred_element_type=jnp.float32)


def angles(place):
    half = HEAD // 2
    angle = place.astype(jnp.float32)[:, None] * THETA ** (-jnp.arange(half, dtype=jnp.float32) / half)
    return jnp.concatenate([jnp.cos(angle), jnp.sin(angle)], 1)


def _normed(x, gain):
    wide = x.astype(jnp.float32)
    scale = lax.rsqrt(jnp.mean(wide * wide, -1, keepdims=True) + 1e-6)
    return (wide * scale * gain).astype(jnp.bfloat16)


def _tables(base, part):
    first = lax.broadcasted_iota(jnp.int32, part.shape, 1) < HEAD // 2
    base = jnp.broadcast_to(base, part.shape)
    base_r, part_r = pltpu.roll(base, HEAD // 2, 1), pltpu.roll(part, HEAD // 2, 1)
    cos_a, sin_a = jnp.where(first, base, base_r), jnp.where(first, base_r, base)
    cos_b, sin_b = jnp.where(first, part, part_r), jnp.where(first, part_r, part)
    cos, sin = cos_a * cos_b - sin_a * sin_b, sin_a * cos_b + cos_a * sin_b
    return cos, jnp.where(first, -sin, sin)


def _turn(t, cos, sin):
    t = t.astype(jnp.bfloat16).astype(jnp.float32)
    return (t * cos + pltpu.roll(t, HEAD // 2, 1) * sin).astype(jnp.bfloat16)


def _kernel(x_ref, gain_ref, wq_ref, wk_ref, wv_ref, base_ref, part_ref, o_ref,
            own, land, wq_s, wk_s, wv_s, q_s, k_s, v_s, a_s, cos_s, sin_s, gap_s, top, mix,
            x_sem, w_sem, pair_send, pair_recv, up_send, link_recv, on_send, side_send, side_recv, o_send, o_recv, o_sem):
    me = lax.axis_index("sp")
    chip, core = lax.div(me, 2), lax.rem(me, 2)
    pair, up, down = chip * 2 + 1 - core, lax.rem(me + 2, 8), lax.rem(me + 6, 8)
    rows = x_ref.shape[0]
    pieces = rows // PIECE
    steps = chip * pieces
    kv, nq = k_s.shape[0], q_s.shape[1]
    g = q_s.shape[2] // BQ
    cols = g * BQ
    mine = kv * HEAD
    e = HEAD**-0.5 * LOG2E

    def remote(src, dst, send, recv, to):
        return pltpu.make_async_remote_copy(src_ref=src, dst_ref=dst, send_sem=send, recv_sem=recv, device_id={"sp": to},
                                            device_id_type=pl.DeviceIdType.MESH)

    own_copy = pltpu.make_async_copy(x_ref, own.at[core], x_sem)
    own_copy.start()
    kv_tiles, q_tiles = wk_s.shape[0], wq_s.shape[0]
    w_copies = []
    for n in range(kv_tiles):
        here = pl.ds(pl.multiple_of(core * mine + n * TILE, TILE), TILE)
        w_copies.append(pltpu.make_async_copy(wk_ref.at[:, here], wk_s.at[n], w_sem.at[2 * n]))
        w_copies.append(pltpu.make_async_copy(wv_ref.at[:, here], wv_s.at[n], w_sem.at[2 * n + 1]))
    for n in range(q_tiles):
        here = pl.ds(pl.multiple_of(core * g * mine + n * TILE, TILE), TILE)
        w_copies.append(pltpu.make_async_copy(wq_ref.at[:, here], wq_s.at[n], w_sem.at[2 * kv_tiles + n]))
    for copy in w_copies:
        copy.start()

    barrier = pltpu.get_barrier_semaphore()
    for other in (pair, up, down):
        pl.semaphore_signal(barrier, inc=1, device_id={"sp": other}, device_id_type=pl.DeviceIdType.MESH)
    pl.semaphore_wait(barrier, 3)

    pair_copy = remote(x_ref, own.at[core], pair_send, pair_recv, pair)
    pair_copy.start()

    def up_copy(n):
        here = pl.ds(n * PIECE, PIECE)
        return remote(x_ref.at[here], land.at[core, n], up_send.at[n], link_recv.at[n], up)

    @pl.when(chip < 3)
    def _():
        for n in range(pieces):
            up_copy(n).start()

    def arrived(t):
        return remote(land.at[core, t], land.at[core, t], on_send.at[t], link_recv.at[t], up)

    def on_copy(t):
        return remote(land.at[core, t], land.at[core, t + pieces], on_send.at[t], link_recv.at[t + pieces], up)

    def side_copy(t):
        return remote(land.at[core, t], land.at[core, t], side_send.at[t], side_recv.at[t], pair)

    def relay(t):
        @pl.when(t < steps)
        def _():
            arrived(t).wait_recv()
            side_copy(t).start()

            @pl.when(chip < 3)
            def _():
                on_copy(t).start()

    gain = gain_ref[...].astype(jnp.float32)

    def turn_own(half):
        cos, sin = _tables(base_ref[pl.ds(chip * 2 + half, 1), :], part_ref[...])
        here = pl.ds(pl.multiple_of(half * rows, rows), rows)
        cos_s[here, :], sin_s[here, :] = cos, sin

    def norm_own(half):
        def some(n, _):
            here = pl.ds(pl.multiple_of(n * PIECE, PIECE), PIECE)
            own[half, here, :] = _normed(own[half, here, :], gain)

        lax.fori_loop(0, pieces, some, None)

    own_copy.wait()
    norm_own(core)
    turn_own(core)
    turn_own(1 - core)
    gap_s[...] = lax.rem(lax.broadcasted_iota(jnp.int32, (BK, cols), 1), BQ) - lax.broadcasted_iota(jnp.int32, (BK, cols), 0)
    top[...] = jnp.full(top.shape, NEG, jnp.float32)
    mix[...] = jnp.zeros(mix.shape, jnp.float32)
    v_s[:, HEAD:, :] = jnp.ones((kv, ONES, v_s.shape[2]), jnp.bfloat16)
    pair_copy.wait_recv()
    norm_own(1 - core)
    for copy in w_copies:
        copy.wait()

    per = TILE // HEAD

    def project_kv(n, a, at, size):
        here = pl.ds(at, size)
        cos, sin = cos_s[here, :], sin_s[here, :]
        k = _dot(a, wk_s[n], 1, 0)
        v = _dot(a, wv_s[n], 1, 0)
        for h in range(per):
            part = slice(h * HEAD, (h + 1) * HEAD)
            k_s[n * per + h, here, :] = _turn(k[:, part], cos, sin)
            v_s[n * per + h, :HEAD, here] = v[:, part].astype(jnp.bfloat16).T

    def own_kv(n, _):
        for half in range(2):
            project_kv(n, own[half], half * rows, rows)

    lax.fori_loop(0, kv_tiles, own_kv, None)

    def own_q(n, _):
        for half in range(2):
            q = _dot(own[half], wq_s[n], 1, 0)
            for b in range(rows // BQ):
                at = half * rows + b * BQ
                cos, sin = cos_s[at : at + BQ, :], sin_s[at : at + BQ, :]
                for h in range(per):
                    head = n * per + h
                    put = pl.ds(pl.multiple_of(lax.rem(head, g) * BQ, BQ), BQ)
                    q_s[lax.div(head, g), half * (rows // BQ) + b, put, :] = _turn(
                        q[b * BQ : (b + 1) * BQ, h * HEAD : (h + 1) * HEAD], cos, sin)

    lax.fori_loop(0, q_tiles, own_q, None)

    for t in range(AHEAD):
        relay(t)

    def block(iq, j, masked):
        here = pl.ds(pl.multiple_of(j * BK, BK), BK)
        scores = [_dot(k_s[i, here, :], q_s[i, iq], 1, 1) for i in range(kv)]
        if masked:
            ok = gap_s[...] >= j * BK - iq * BQ
        weights, keeps = [], []
        for i, s in enumerate(scores):
            if masked:
                s = jnp.where(ok, s, HIDDEN)
            old = top[iq, i : i + 1, :]
            new = jnp.maximum(old, s.max(axis=0, keepdims=True))
            top[iq, i : i + 1, :] = new
            weights.append(jnp.exp2((s - new) * e).astype(jnp.bfloat16))
            keeps.append(jnp.exp2((old - new) * e))
        for i, (p, keep) in enumerate(zip(weights, keeps)):
            mix[iq, i] = mix[iq, i] * keep + _dot(v_s[i, :, here], p, 1, 0)

    def own_block(iq, _):
        lax.fori_loop(0, iq, lambda j, _: block(iq, j, False), None)
        block(iq, iq, True)

    lax.fori_loop(0, nq, own_block, None)

    def step(t, _):
        relay(t + AHEAD)
        side_copy(t).wait_recv()
        source = chip - 1 - lax.div(t, pieces)
        at = pl.multiple_of(lax.rem(t, pieces) * PIECE, PIECE)
        for half in range(2):
            here = slice(half * PIECE, (half + 1) * PIECE)
            a_s[here, :] = _normed(land[half, t], gain)
            cos_s[here, :], sin_s[here, :] = _tables(base_ref[pl.ds(source * 2 + half, 1), :], part_ref[pl.ds(at, PIECE), :])
        lax.fori_loop(0, kv_tiles, lambda n, _: project_kv(n, a_s[...], 0, BK), None)
        lax.fori_loop(0, nq, lambda iq, _: block(iq, 0, False), None)

    lax.fori_loop(0, steps, step, None)

    def o_copy(u):
        here = pl.ds(u * BQ, BQ)
        to = pl.ds(pl.multiple_of(core * g * mine, g * mine), g * mine)
        return remote(own.at[1 - core, here], o_ref.at[here, to], o_send.at[u], o_recv.at[u], pair)

    def o_keep(u):
        here = pl.ds(u * BQ, BQ)
        to = pl.ds(pl.multiple_of(core * g * mine, g * mine), g * mine)
        return pltpu.make_async_copy(own.at[core, here], o_ref.at[here, to], o_sem.at[u])

    copies = [o_copy(0), o_copy(1), o_keep(0), o_keep(1)]
    for u in range(4):
        half = 1 - core if u < 2 else core
        iq = half * 2 + u % 2
        for i in range(kv):
            out = mix[iq, i, :HEAD, :] * (1 / mix[iq, i, HEAD : HEAD + 1, :])
            for n in range(g):
                at = (i * g + n) * HEAD
                own[half, (u % 2) * BQ : (u % 2 + 1) * BQ, at : at + HEAD] = out[:, n * BQ : (n + 1) * BQ].T.astype(jnp.bfloat16)
        if u:
            copies[u - 1].start()
    copies[3].start()

    pair_copy.wait_send()

    @pl.when(chip < 3)
    def _():
        for n in range(pieces):
            up_copy(n).wait_send()

    def sent(t, _):
        side_copy(t).wait_send()

        @pl.when(chip < 3)
        def _():
            on_copy(t).wait_send()

    lax.fori_loop(0, steps, sent, None)
    for u in range(2):
        copies[u].wait()
        copies[2 + u].wait()


def attention(x, gain, wq, wk, wv, base, part):
    rows, depth = x.shape
    kv = wk.shape[1] // HEAD // 2
    heads = wq.shape[1] // HEAD // 2
    g = heads // kv
    tokens = 2 * rows
    pieces = rows // PIECE
    far = 3 * pieces
    nq = tokens // BQ
    low = jnp.bfloat16
    anywhere = pl.BlockSpec(memory_space=pl.ANY)
    held = pl.BlockSpec(memory_space=pltpu.VMEM)
    dma = pltpu.SemaphoreType.DMA
    return pl.pallas_call(
        _kernel,
        in_specs=[anywhere, held, anywhere, anywhere, anywhere, held, held],
        out_specs=anywhere,
        out_shape=jax.ShapeDtypeStruct((rows, 2 * heads * HEAD), low),
        scratch_shapes=[
            pltpu.VMEM((2, rows, depth), low),
            pltpu.VMEM((2, far, PIECE, depth), low),
            pltpu.VMEM((heads * HEAD // TILE, depth, TILE), low),
            pltpu.VMEM((kv * HEAD // TILE, depth, TILE), low),
            pltpu.VMEM((kv * HEAD // TILE, depth, TILE), low),
            pltpu.VMEM((kv, nq, g * BQ, HEAD), low),
            pltpu.VMEM((kv, tokens, HEAD), low),
            pltpu.VMEM((kv, HEAD + ONES, tokens), low),
            pltpu.VMEM((BK, depth), low),
            pltpu.VMEM((tokens, HEAD), jnp.float32),
            pltpu.VMEM((tokens, HEAD), jnp.float32),
            pltpu.VMEM((BK, g * BQ), jnp.int32),
            pltpu.VMEM((nq, kv, g * BQ), jnp.float32),
            pltpu.VMEM((nq, kv, HEAD + ONES, g * BQ), jnp.float32),
            dma, dma((2 * kv * HEAD // TILE + heads * HEAD // TILE,)), dma, dma,
            dma((pieces,)), dma((far,)), dma((far,)), dma((far,)), dma((far,)),
            dma((2,)), dma((2,)), dma((2,)),
        ],
        compiler_params=pltpu.CompilerParams(collective_id=0, has_side_effects=True, vmem_limit_bytes=VMEM),
        name="attention",
    )(x, gain[None], wq, wk, wv, base, part)


def solution(mesh):
    devices = mesh.shape["sp"]

    def step(x, gain, wq, wk, wv, wo):
        rows = x.shape[0]
        base, part = angles(jnp.arange(devices) * rows), angles(jnp.arange(rows))
        o = attention(x, gain, wq, wk, wv, base, part)
        y = jnp.dot(o, wo, preferred_element_type=jnp.float32)
        return (x.astype(jnp.float32) + y).astype(jnp.bfloat16)

    tokens, whole = P(("dp", "sp"), None), P(None, None)
    return jax.shard_map(
        step,
        mesh=mesh,
        in_specs=(tokens, P(None), whole, whole, whole, whole),
        out_specs=tokens,
        check_vma=False,
    )
```

```python
import functools

import jax
import jax.numpy as jnp
import numpy as np
from jax import lax
from jax.experimental import pallas as pl
from jax.experimental.pallas import tpu as pltpu
from jax.sharding import PartitionSpec as P

HEAD = 128
THETA = 10000
NEG = -1e30
HIDDEN = 2 * NEG
LOG2E = 1.4426950408889634
VMEM = 63 * 2**20
ONES = 8
PIECE = 128
BQ = 256
BK = 256
PAIR = 2
AT_ONCE = 4
TILE = 256


def _dot(a, b, ca, cb):
    return lax.dot_general(a, b, (((ca,), (cb,)), ((), ())), preferred_element_type=jnp.float32)


def angles(place):
    half = HEAD // 2
    angle = place[:, None] * float(THETA) ** (-np.arange(half) / half)
    return jnp.asarray(np.concatenate([np.cos(angle), np.sin(angle)], 1), jnp.float32)


def _normed(x, gain):
    wide = x.astype(jnp.float32)
    scale = lax.rsqrt(jnp.mean(wide * wide, -1, keepdims=True) + 1e-6)
    return (wide * scale * gain).astype(jnp.bfloat16)


def _tables(base, part):
    first = lax.broadcasted_iota(jnp.int32, part.shape, 1) < HEAD // 2
    base = jnp.broadcast_to(base, part.shape)
    base_r, part_r = pltpu.roll(base, HEAD // 2, 1), pltpu.roll(part, HEAD // 2, 1)
    cos_a, sin_a = jnp.where(first, base, base_r), jnp.where(first, base_r, base)
    cos_b, sin_b = jnp.where(first, part, part_r), jnp.where(first, part_r, part)
    cos, sin = cos_a * cos_b - sin_a * sin_b, sin_a * cos_b + cos_a * sin_b
    return cos, jnp.where(first, -sin, sin)


def _turn(t, cos, sin):
    t = t.astype(jnp.bfloat16).astype(jnp.float32)
    return (t * cos + pltpu.roll(t, HEAD // 2, 1) * sin).astype(jnp.bfloat16)


def _kernel(x_ref, gain_ref, wq_ref, wk_ref, wv_ref, base_ref, part_ref, o_ref,
            own, land, wq_s, wk_s, wv_s, q_s, k_s, v_s, a_s, cos_s, sin_s, gap_s, top, mix,
            x_sem, w_sem, pair_send, pair_recv, up_send, link_recv, on_send, side_send, side_recv, o_send, o_recv, o_sem):
    me = lax.axis_index("sp")
    chip, core = lax.div(me, 2), lax.rem(me, 2)
    pair, up, down = chip * 2 + 1 - core, lax.rem(me + 2, 8), lax.rem(me + 6, 8)
    rows = x_ref.shape[0]
    pieces = rows // PIECE
    steps = chip * pieces
    kv, nq = k_s.shape[0], q_s.shape[1]
    g = q_s.shape[2] // BQ
    cols = g * BQ
    mine = kv * HEAD
    e = HEAD**-0.5 * LOG2E

    def remote(src, dst, send, recv, to):
        return pltpu.make_async_remote_copy(src_ref=src, dst_ref=dst, send_sem=send, recv_sem=recv, device_id={"sp": to},
                                            device_id_type=pl.DeviceIdType.MESH)

    own_copy = pltpu.make_async_copy(x_ref, own.at[core], x_sem)
    own_copy.start()
    kv_tiles, q_tiles = wk_s.shape[0], wq_s.shape[0]
    w_copies = []
    for n in range(kv_tiles):
        here = pl.ds(pl.multiple_of(core * mine + n * TILE, TILE), TILE)
        w_copies.append(pltpu.make_async_copy(wk_ref.at[:, here], wk_s.at[n], w_sem.at[2 * n]))
        w_copies.append(pltpu.make_async_copy(wv_ref.at[:, here], wv_s.at[n], w_sem.at[2 * n + 1]))
    for n in range(q_tiles):
        here = pl.ds(pl.multiple_of(core * g * mine + n * TILE, TILE), TILE)
        w_copies.append(pltpu.make_async_copy(wq_ref.at[:, here], wq_s.at[n], w_sem.at[2 * kv_tiles + n]))
    for copy in w_copies:
        copy.start()

    barrier = pltpu.get_barrier_semaphore()
    for other in (pair, up, down):
        pl.semaphore_signal(barrier, inc=1, device_id={"sp": other}, device_id_type=pl.DeviceIdType.MESH)
    pl.semaphore_wait(barrier, 3)

    pair_copy = remote(x_ref, own.at[core], pair_send, pair_recv, pair)
    pair_copy.start()

    def up_copy(n):
        here = pl.ds(n * PIECE, PIECE)
        return remote(x_ref.at[here], land.at[core, n], up_send.at[n], link_recv.at[n], up)

    @pl.when(chip < 3)
    def _():
        for n in range(pieces):
            up_copy(n).start()

    def arrived(t):
        return remote(land.at[core, t], land.at[core, t], on_send.at[t], link_recv.at[t], up)

    def on_copy(t):
        return remote(land.at[core, t], land.at[core, t + pieces], on_send.at[t], link_recv.at[t + pieces], up)

    def side_copy(t):
        return remote(land.at[core, t], land.at[core, t], side_send.at[t], side_recv.at[t], pair)

    def relay(t):
        @pl.when(t < steps)
        def _():
            arrived(t).wait_recv()
            side_copy(t).start()

            @pl.when(chip < 3)
            def _():
                on_copy(t).start()

    gain = gain_ref[...].astype(jnp.float32)[None]

    def turn_own(half):
        cos, sin = _tables(base_ref[pl.ds(chip * 2 + half, 1), :], part_ref[...])
        here = pl.ds(pl.multiple_of(half * rows, rows), rows)
        cos_s[here, :], sin_s[here, :] = cos, sin

    def norm_own(half):
        def some(n, _):
            here = pl.ds(pl.multiple_of(n * PIECE, PIECE), PIECE)
            own[half, here, :] = _normed(own[half, here, :], gain)

        lax.fori_loop(0, pieces, some, None)

    own_copy.wait()
    norm_own(core)
    turn_own(core)
    turn_own(1 - core)
    gap_s[...] = lax.rem(lax.broadcasted_iota(jnp.int32, (BK, cols), 1), BQ) - lax.broadcasted_iota(jnp.int32, (BK, cols), 0)
    top[...] = jnp.full(top.shape, NEG, jnp.float32)
    mix[...] = jnp.zeros(mix.shape, jnp.float32)
    v_s[:, HEAD:, :] = jnp.ones((kv, ONES, v_s.shape[2]), jnp.bfloat16)
    pair_copy.wait_recv()
    norm_own(1 - core)
    for copy in w_copies:
        copy.wait()

    per = TILE // HEAD

    def project_kv(n, a, at, size):
        here = pl.ds(at, size)
        cos, sin = cos_s[here, :], sin_s[here, :]
        k = _dot(a, wk_s[n], 1, 0)
        v = _dot(a, wv_s[n], 1, 0)
        for h in range(per):
            part = slice(h * HEAD, (h + 1) * HEAD)
            k_s[n * per + h, here, :] = _turn(k[:, part], cos, sin)
            v_s[n * per + h, :HEAD, here] = v[:, part].astype(jnp.bfloat16).T

    def own_kv(n, _):
        for half in range(2):
            project_kv(n, own[half], half * rows, rows)

    lax.fori_loop(0, kv_tiles, own_kv, None)

    def own_q(n, _):
        for half in range(2):
            q = _dot(own[half], wq_s[n], 1, 0)
            for b in range(rows // BQ):
                at = half * rows + b * BQ
                cos, sin = cos_s[at : at + BQ, :], sin_s[at : at + BQ, :]
                for h in range(per):
                    head = n * per + h
                    put = pl.ds(pl.multiple_of(lax.rem(head, g) * BQ, BQ), BQ)
                    q_s[lax.div(head, g), half * (rows // BQ) + b, put, :] = _turn(
                        q[b * BQ : (b + 1) * BQ, h * HEAD : (h + 1) * HEAD], cos, sin)

    lax.fori_loop(0, q_tiles, own_q, None)

    def relays(first, end):
        lax.fori_loop(first, end, lambda t, _: relay(t), None)

    relays(0, 2)

    def block(iq, first, size, masked):
        here = pl.ds(first, size)
        for group in range(0, kv, AT_ONCE):
            heads = range(group, group + AT_ONCE)
            scores = [_dot(k_s[i, here, :], q_s[i, iq], 1, 1) for i in heads]
            if masked:
                ok = gap_s[...] >= first - iq * BQ
            weights, keeps = [], []
            for i, s in zip(heads, scores):
                if masked:
                    s = jnp.where(ok, s, HIDDEN)
                old = top[iq, i : i + 1, :]
                new = jnp.maximum(old, s.max(axis=0, keepdims=True))
                top[iq, i : i + 1, :] = new
                weights.append(jnp.exp2((s - new) * e).astype(jnp.bfloat16))
                keeps.append(jnp.exp2((old - new) * e))
            for i, p, keep in zip(heads, weights, keeps):
                mix[iq, i] = mix[iq, i] * keep + _dot(v_s[i, :, here], p, 1, 0)

    def own_block(iq, _):
        lax.fori_loop(0, iq, lambda j, _: block(iq, pl.multiple_of(j * BK, BK), BK, False), None)
        block(iq, pl.multiple_of(iq * BK, BK), BK, True)

    lax.fori_loop(0, nq, own_block, None)

    def step(t, count, relay_between):
        for n in range(count):
            side_copy(t + n).wait_recv()
        source = chip - 1 - lax.div(t, pieces)
        for half in range(2):
            for n in range(count):
                at = pl.multiple_of(lax.rem(t + n, pieces) * PIECE, PIECE)
                here = slice((half * count + n) * PIECE, (half * count + n + 1) * PIECE)
                a_s[here, :] = _normed(land[half, t + n], gain)
                cos_s[here, :], sin_s[here, :] = _tables(base_ref[pl.ds(source * 2 + half, 1), :], part_ref[pl.ds(at, PIECE), :])
        keys = 2 * count * PIECE
        lax.fori_loop(0, kv_tiles, lambda n, _: project_kv(n, a_s[:keys, :], 0, keys), None)
        relay_between()
        lax.fori_loop(0, nq, lambda iq, _: block(iq, 0, keys, False), None)

    def due(u):
        return jnp.where(chip < 3, 2 * u + 4, 2 * u + 2 + jnp.where(u < 2, 1, 0))

    def between(u):
        return due(u) + jnp.where((chip == 3) & ((u == 0) | (u == 2)), 1, 0)

    def double(u, _):
        relays(jnp.where(u == 0, 2, between(u - 1)), due(u))
        step(u * 2, 2, lambda: relays(due(u), between(u)))

    doubles = chip * (pieces // 2) - jnp.where(chip == 3, 1, 0)
    lax.fori_loop(0, doubles, double, None)

    def single(t, _):
        relay(t)
        step(t, 1, lambda: None)

    lax.fori_loop(doubles * 2, steps, single, None)

    def o_copy(u):
        here = pl.ds(u * BQ, BQ)
        to = pl.ds(pl.multiple_of(core * g * mine, g * mine), g * mine)
        return remote(own.at[1 - core, here], o_ref.at[here, to], o_send.at[u], o_recv.at[u], pair)

    def o_keep(u):
        here = pl.ds(u * BQ, BQ)
        to = pl.ds(pl.multiple_of(core * g * mine, g * mine), g * mine)
        return pltpu.make_async_copy(own.at[core, here], o_ref.at[here, to], o_sem.at[u])

    copies = [o_copy(0), o_copy(1), o_keep(0), o_keep(1)]
    for u in range(4):
        half = 1 - core if u < 2 else core
        iq = half * 2 + u % 2
        for i in range(kv):
            out = mix[iq, i, :HEAD, :] * (1 / mix[iq, i, HEAD : HEAD + 1, :])
            for n in range(g):
                at = (i * g + n) * HEAD
                own[half, (u % 2) * BQ : (u % 2 + 1) * BQ, at : at + HEAD] = out[:, n * BQ : (n + 1) * BQ].T.astype(jnp.bfloat16)
        if u:
            copies[u - 1].start()
    copies[3].start()

    pair_copy.wait_send()

    @pl.when(chip < 3)
    def _():
        for n in range(pieces):
            up_copy(n).wait_send()

    def sent(t, _):
        side_copy(t).wait_send()

        @pl.when(chip < 3)
        def _():
            on_copy(t).wait_send()

    lax.fori_loop(0, steps, sent, None)
    for u in range(2):
        copies[u].wait()
        copies[2 + u].wait()


def attention(x, gain, wq, wk, wv, base, part):
    rows, depth = x.shape
    kv = wk.shape[1] // HEAD // 2
    heads = wq.shape[1] // HEAD // 2
    g = heads // kv
    tokens = 2 * rows
    pieces = rows // PIECE
    far = 3 * pieces
    nq = tokens // BQ
    low = jnp.bfloat16
    anywhere = pl.BlockSpec(memory_space=pl.ANY)
    held = pl.BlockSpec(memory_space=pltpu.VMEM)
    dma = pltpu.SemaphoreType.DMA
    return pl.pallas_call(
        _kernel,
        in_specs=[anywhere, held, anywhere, anywhere, anywhere, held, held],
        out_specs=anywhere,
        out_shape=jax.ShapeDtypeStruct((rows, 2 * heads * HEAD), low),
        scratch_shapes=[
            pltpu.VMEM((2, rows, depth), low),
            pltpu.VMEM((2, far, PIECE, depth), low),
            pltpu.VMEM((heads * HEAD // TILE, depth, TILE), low),
            pltpu.VMEM((kv * HEAD // TILE, depth, TILE), low),
            pltpu.VMEM((kv * HEAD // TILE, depth, TILE), low),
            pltpu.VMEM((kv, nq, g * BQ, HEAD), low),
            pltpu.VMEM((kv, tokens, HEAD), low),
            pltpu.VMEM((kv, HEAD + ONES, tokens), low),
            pltpu.VMEM((2 * PAIR * PIECE, depth), low),
            pltpu.VMEM((tokens, HEAD), jnp.float32),
            pltpu.VMEM((tokens, HEAD), jnp.float32),
            pltpu.VMEM((BK, g * BQ), jnp.int32),
            pltpu.VMEM((nq, kv, g * BQ), jnp.float32),
            pltpu.VMEM((nq, kv, HEAD + ONES, g * BQ), jnp.float32),
            dma, dma((2 * kv * HEAD // TILE + heads * HEAD // TILE,)), dma, dma,
            dma((pieces,)), dma((far,)), dma((far,)), dma((far,)), dma((far,)),
            dma((2,)), dma((2,)), dma((2,)),
        ],
        compiler_params=pltpu.CompilerParams(collective_id=0, has_side_effects=True, vmem_limit_bytes=VMEM),
        name="attention",
    )(x, gain, wq, wk, wv, base, part)


def solution(mesh):
    devices = mesh.shape["sp"]

    def step(x, gain, wq, wk, wv, wo):
        rows = x.shape[0]
        base, part = angles(np.arange(devices) * rows), angles(np.arange(rows))
        o = attention(x, gain, wq, wk, wv, base, part)
        y = jnp.dot(o, wo, preferred_element_type=jnp.float32)
        return (x.astype(jnp.float32) + y).astype(jnp.bfloat16)

    tokens, whole = P(("dp", "sp"), None), P(None, None)
    return jax.shard_map(
        step,
        mesh=mesh,
        in_specs=(tokens, P(None), whole, whole, whole, whole),
        out_specs=tokens,
        check_vma=False,
    )
```

```python
import functools

import jax
import jax.numpy as jnp
import numpy as np
from jax import lax
from jax.experimental import pallas as pl
from jax.experimental.pallas import tpu as pltpu
from jax.sharding import PartitionSpec as P

HEAD = 128
THETA = 10000
NEG = -1e30
HIDDEN = 2 * NEG
LOG2E = 1.4426950408889634
VMEM = 63 * 2**20
ONES = 8
PIECE = 128
BQ = 256
BK = 256
PAIR = 2
AT_ONCE = 8
TILE = 256


def _dot(a, b, ca, cb):
    return lax.dot_general(a, b, (((ca,), (cb,)), ((), ())), preferred_element_type=jnp.float32)


def angles(place):
    half = HEAD // 2
    angle = place[:, None] * float(THETA) ** (-np.arange(half) / half)
    return jnp.asarray(np.concatenate([np.cos(angle), np.sin(angle)], 1), jnp.float32)


def _normed(x, gain):
    wide = x.astype(jnp.float32)
    scale = lax.rsqrt(jnp.mean(wide * wide, -1, keepdims=True) + 1e-6)
    return (wide * scale * gain).astype(jnp.bfloat16)


def _tables(base, part):
    first = lax.broadcasted_iota(jnp.int32, part.shape, 1) < HEAD // 2
    base = jnp.broadcast_to(base, part.shape)
    base_r, part_r = pltpu.roll(base, HEAD // 2, 1), pltpu.roll(part, HEAD // 2, 1)
    cos_a, sin_a = jnp.where(first, base, base_r), jnp.where(first, base_r, base)
    cos_b, sin_b = jnp.where(first, part, part_r), jnp.where(first, part_r, part)
    cos, sin = cos_a * cos_b - sin_a * sin_b, sin_a * cos_b + cos_a * sin_b
    return cos, jnp.where(first, -sin, sin)


def _turn(t, cos, sin):
    t = t.astype(jnp.bfloat16).astype(jnp.float32)
    return (t * cos + pltpu.roll(t, HEAD // 2, 1) * sin).astype(jnp.bfloat16)


def _kernel(x_ref, gain_ref, wq_ref, wk_ref, wv_ref, base_ref, part_ref, o_ref,
            own, land, wq_s, wk_s, wv_s, q_s, k_s, v_s, a_s, cos_s, sin_s, gap_s, top, mix,
            x_sem, w_sem, pair_send, pair_recv, up_send, link_recv, on_send, side_send, side_recv, o_send, o_recv, o_sem):
    me = lax.axis_index("sp")
    chip, core = lax.div(me, 2), lax.rem(me, 2)
    pair, up, down = chip * 2 + 1 - core, lax.rem(me + 2, 8), lax.rem(me + 6, 8)
    rows = x_ref.shape[0]
    pieces = rows // PIECE
    steps = chip * pieces
    kv, nq = k_s.shape[0], q_s.shape[1]
    g = q_s.shape[2] // BQ
    cols = g * BQ
    mine = kv * HEAD
    e = HEAD**-0.5 * LOG2E

    def remote(src, dst, send, recv, to):
        return pltpu.make_async_remote_copy(src_ref=src, dst_ref=dst, send_sem=send, recv_sem=recv, device_id={"sp": to},
                                            device_id_type=pl.DeviceIdType.MESH)

    own_copy = pltpu.make_async_copy(x_ref, own.at[core], x_sem)
    own_copy.start()
    kv_tiles, q_tiles = wk_s.shape[0], wq_s.shape[0]

    def kv_copies(n):
        here = pl.ds(pl.multiple_of(core * mine + n * TILE, TILE), TILE)
        return [pltpu.make_async_copy(wk_ref.at[:, here], wk_s.at[n], w_sem.at[2 * n]),
                pltpu.make_async_copy(wv_ref.at[:, here], wv_s.at[n], w_sem.at[2 * n + 1])]

    def q_copy(n):
        here = pl.ds(pl.multiple_of(core * g * mine + n * TILE, TILE), TILE)
        return pltpu.make_async_copy(wq_ref.at[:, here], wq_s.at[n], w_sem.at[2 * kv_tiles + n])

    for n in range(kv_tiles):
        for copy in kv_copies(n):
            copy.start()
    for n in range(q_tiles):
        q_copy(n).start()

    barrier = pltpu.get_barrier_semaphore()
    for other in (pair, up, down):
        pl.semaphore_signal(barrier, inc=1, device_id={"sp": other}, device_id_type=pl.DeviceIdType.MESH)
    pl.semaphore_wait(barrier, 3)

    pair_copy = remote(x_ref, own.at[core], pair_send, pair_recv, pair)
    pair_copy.start()

    def up_copy(n):
        here = pl.ds(n * PIECE, PIECE)
        return remote(x_ref.at[here], land.at[core, n], up_send.at[n], link_recv.at[n], up)

    @pl.when(chip < 3)
    def _():
        for n in range(pieces):
            up_copy(n).start()

    def arrived(t):
        return remote(land.at[core, t], land.at[core, t], on_send.at[t], link_recv.at[t], up)

    def on_copy(t):
        return remote(land.at[core, t], land.at[core, t + pieces], on_send.at[t], link_recv.at[t + pieces], up)

    def side_copy(t):
        return remote(land.at[core, t], land.at[core, t], side_send.at[t], side_recv.at[t], pair)

    def relay(t):
        @pl.when(t < steps)
        def _():
            arrived(t).wait_recv()
            side_copy(t).start()

            @pl.when(chip < 3)
            def _():
                on_copy(t).start()

    gain = gain_ref[...].astype(jnp.float32)[None]

    def turn_own(half):
        cos, sin = _tables(base_ref[pl.ds(chip * 2 + half, 1), :], part_ref[...])
        here = pl.ds(pl.multiple_of(half * rows, rows), rows)
        cos_s[here, :], sin_s[here, :] = cos, sin

    def norm_own(half):
        def some(n, _):
            here = pl.ds(pl.multiple_of(n * PIECE, PIECE), PIECE)
            own[half, here, :] = _normed(own[half, here, :], gain)

        lax.fori_loop(0, pieces, some, None)

    own_copy.wait()
    norm_own(core)
    turn_own(core)
    turn_own(1 - core)
    gap_s[...] = lax.rem(lax.broadcasted_iota(jnp.int32, (BK, cols), 1), BQ) - lax.broadcasted_iota(jnp.int32, (BK, cols), 0)
    top[...] = jnp.full(top.shape, NEG, jnp.float32)
    mix[...] = jnp.zeros(mix.shape, jnp.float32)
    v_s[:, HEAD:, :] = jnp.ones((kv, ONES, v_s.shape[2]), jnp.bfloat16)
    pair_copy.wait_recv()
    norm_own(1 - core)
    per = TILE // HEAD

    def project_kv(n, a, at, size):
        here = pl.ds(at, size)
        cos, sin = cos_s[here, :], sin_s[here, :]
        k = _dot(a, wk_s[n], 1, 0)
        v = _dot(a, wv_s[n], 1, 0)
        for h in range(per):
            part = slice(h * HEAD, (h + 1) * HEAD)
            k_s[n * per + h, here, :] = _turn(k[:, part], cos, sin)
            v_s[n * per + h, :HEAD, here] = v[:, part].astype(jnp.bfloat16).T

    def own_kv(n, _):
        for copy in kv_copies(n):
            copy.wait()
        for half in range(2):
            project_kv(n, own[half], half * rows, rows)

    lax.fori_loop(0, kv_tiles, own_kv, None)

    def own_q(n, _):
        q_copy(n).wait()
        for half in range(2):
            q = _dot(own[half], wq_s[n], 1, 0)
            for b in range(rows // BQ):
                at = half * rows + b * BQ
                cos, sin = cos_s[at : at + BQ, :], sin_s[at : at + BQ, :]
                for h in range(per):
                    head = n * per + h
                    put = pl.ds(pl.multiple_of(lax.rem(head, g) * BQ, BQ), BQ)
                    q_s[lax.div(head, g), half * (rows // BQ) + b, put, :] = _turn(
                        q[b * BQ : (b + 1) * BQ, h * HEAD : (h + 1) * HEAD], cos, sin)

    def own_q_twice(n, _):
        own_q(2 * n, None)
        own_q(2 * n + 1, None)

    lax.fori_loop(0, q_tiles // 2, own_q_twice, None)

    def relays(first, end):
        lax.fori_loop(first, end, lambda t, _: relay(t), None)

    relays(0, 2)

    def block(iq, first, size, masked):
        here = pl.ds(first, size)
        for group in range(0, kv, AT_ONCE):
            heads = range(group, group + AT_ONCE)
            scores = [_dot(k_s[i, here, :], q_s[i, iq], 1, 1) for i in heads]
            if masked:
                ok = gap_s[...] >= first - iq * BQ
            weights, keeps = [], []
            for i, s in zip(heads, scores):
                if masked:
                    s = jnp.where(ok, s, HIDDEN)
                old = top[iq, i : i + 1, :]
                new = jnp.maximum(old, s.max(axis=0, keepdims=True))
                top[iq, i : i + 1, :] = new
                weights.append(jnp.exp2((s - new) * e).astype(jnp.bfloat16))
                keeps.append(jnp.exp2((old - new) * e))
            for i, p, keep in zip(heads, weights, keeps):
                mix[iq, i] = mix[iq, i] * keep + _dot(v_s[i, :, here], p, 1, 0)

    def own_block(iq, _):
        lax.fori_loop(0, iq, lambda j, _: block(iq, pl.multiple_of(j * BK, BK), BK, False), None)
        block(iq, pl.multiple_of(iq * BK, BK), BK, True)

    lax.fori_loop(0, nq, own_block, None)

    def step(t, count, relay_between):
        for n in range(count):
            side_copy(t + n).wait_recv()
        source = chip - 1 - lax.div(t, pieces)
        for half in range(2):
            for n in range(count):
                at = pl.multiple_of(lax.rem(t + n, pieces) * PIECE, PIECE)
                here = slice((half * count + n) * PIECE, (half * count + n + 1) * PIECE)
                a_s[here, :] = _normed(land[half, t + n], gain)
                cos_s[here, :], sin_s[here, :] = _tables(base_ref[pl.ds(source * 2 + half, 1), :], part_ref[pl.ds(at, PIECE), :])
        keys = 2 * count * PIECE

        def some(n, _):
            for m in range(2):
                project_kv(2 * n + m, a_s[:keys, :], 0, keys)

        lax.fori_loop(0, kv_tiles // 2, some, None)
        relay_between()
        lax.fori_loop(0, nq, lambda iq, _: block(iq, 0, keys, False), None)

    def due(u):
        return jnp.where(chip < 3, 2 * u + 4, 2 * u + 2 + jnp.where(u < 2, 1, 0))

    def between(u):
        return due(u) + jnp.where((chip == 3) & ((u == 0) | (u == 2)), 1, 0)

    def double(u, _):
        relays(jnp.where(u == 0, 2, between(u - 1)), due(u))
        step(u * 2, 2, lambda: relays(due(u), between(u)))

    doubles = chip * (pieces // 2) - jnp.where(chip == 3, 1, 0)
    lax.fori_loop(0, doubles, double, None)

    def single(t, _):
        relay(t)
        step(t, 1, lambda: None)

    lax.fori_loop(doubles * 2, steps, single, None)

    def o_copy(u):
        here = pl.ds(u * BQ, BQ)
        to = pl.ds(pl.multiple_of(core * g * mine, g * mine), g * mine)
        return remote(own.at[1 - core, here], o_ref.at[here, to], o_send.at[u], o_recv.at[u], pair)

    def o_keep(u):
        here = pl.ds(u * BQ, BQ)
        to = pl.ds(pl.multiple_of(core * g * mine, g * mine), g * mine)
        return pltpu.make_async_copy(own.at[core, here], o_ref.at[here, to], o_sem.at[u])

    copies = [o_copy(0), o_copy(1), o_keep(0), o_keep(1)]
    for u in range(4):
        half = 1 - core if u < 2 else core
        iq = half * 2 + u % 2
        for i in range(kv):
            out = mix[iq, i, :HEAD, :] * (1 / mix[iq, i, HEAD : HEAD + 1, :])
            for n in range(g):
                at = (i * g + n) * HEAD
                own[half, (u % 2) * BQ : (u % 2 + 1) * BQ, at : at + HEAD] = out[:, n * BQ : (n + 1) * BQ].T.astype(jnp.bfloat16)
        if u:
            copies[u - 1].start()
    copies[3].start()

    pair_copy.wait_send()

    @pl.when(chip < 3)
    def _():
        for n in range(pieces):
            up_copy(n).wait_send()

    def sent(t, _):
        side_copy(t).wait_send()

        @pl.when(chip < 3)
        def _():
            on_copy(t).wait_send()

    lax.fori_loop(0, steps, sent, None)
    for u in range(2):
        copies[u].wait()
        copies[2 + u].wait()


def attention(x, gain, wq, wk, wv, base, part):
    rows, depth = x.shape
    kv = wk.shape[1] // HEAD // 2
    heads = wq.shape[1] // HEAD // 2
    g = heads // kv
    tokens = 2 * rows
    pieces = rows // PIECE
    far = 3 * pieces
    nq = tokens // BQ
    low = jnp.bfloat16
    anywhere = pl.BlockSpec(memory_space=pl.ANY)
    held = pl.BlockSpec(memory_space=pltpu.VMEM)
    dma = pltpu.SemaphoreType.DMA
    return pl.pallas_call(
        _kernel,
        in_specs=[anywhere, held, anywhere, anywhere, anywhere, held, held],
        out_specs=anywhere,
        out_shape=jax.ShapeDtypeStruct((rows, 2 * heads * HEAD), low),
        scratch_shapes=[
            pltpu.VMEM((2, rows, depth), low),
            pltpu.VMEM((2, far, PIECE, depth), low),
            pltpu.VMEM((heads * HEAD // TILE, depth, TILE), low),
            pltpu.VMEM((kv * HEAD // TILE, depth, TILE), low),
            pltpu.VMEM((kv * HEAD // TILE, depth, TILE), low),
            pltpu.VMEM((kv, nq, g * BQ, HEAD), low),
            pltpu.VMEM((kv, tokens, HEAD), low),
            pltpu.VMEM((kv, HEAD + ONES, tokens), low),
            pltpu.VMEM((2 * PAIR * PIECE, depth), low),
            pltpu.VMEM((tokens, HEAD), jnp.float32),
            pltpu.VMEM((tokens, HEAD), jnp.float32),
            pltpu.VMEM((BK, g * BQ), jnp.int32),
            pltpu.VMEM((nq, kv, g * BQ), jnp.float32),
            pltpu.VMEM((nq, kv, HEAD + ONES, g * BQ), jnp.float32),
            dma, dma((2 * kv * HEAD // TILE + heads * HEAD // TILE,)), dma, dma,
            dma((pieces,)), dma((far,)), dma((far,)), dma((far,)), dma((far,)),
            dma((2,)), dma((2,)), dma((2,)),
        ],
        compiler_params=pltpu.CompilerParams(collective_id=0, has_side_effects=True, vmem_limit_bytes=VMEM),
        name="attention",
    )(x, gain, wq, wk, wv, base, part)


def solution(mesh):
    devices = mesh.shape["sp"]

    def step(x, gain, wq, wk, wv, wo):
        rows = x.shape[0]
        base, part = angles(np.arange(devices) * rows), angles(np.arange(rows))
        o = attention(x, gain, wq, wk, wv, base, part)
        y = jnp.dot(o, wo, preferred_element_type=jnp.float32)
        return (x.astype(jnp.float32) + y).astype(jnp.bfloat16)

    tokens, whole = P(("dp", "sp"), None), P(None, None)
    return jax.shard_map(
        step,
        mesh=mesh,
        in_specs=(tokens, P(None), whole, whole, whole, whole),
        out_specs=tokens,
        check_vma=False,
    )
```

```python
import functools

import jax
import jax.numpy as jnp
import numpy as np
from jax import lax
from jax.experimental import pallas as pl
from jax.experimental.pallas import tpu as pltpu
from jax.sharding import PartitionSpec as P

HEAD = 128
THETA = 10000
NEG = -1e30
HIDDEN = 2 * NEG
LOG2E = 1.4426950408889634
VMEM = 63 * 2**20
ONES = 8
PIECE = 128
BQ = 256
BK = 256
PAIR = 2
AT_ONCE = 8
TILE = 256


def _dot(a, b, ca, cb):
    return lax.dot_general(a, b, (((ca,), (cb,)), ((), ())), preferred_element_type=jnp.float32)


def angles(place):
    half = HEAD // 2
    angle = place[:, None] * float(THETA) ** (-np.arange(half) / half)
    return jnp.asarray(np.concatenate([np.cos(angle), np.sin(angle)], 1), jnp.float32)


def _normed(x, gain):
    wide = x.astype(jnp.float32)
    scale = lax.rsqrt(jnp.mean(wide * wide, -1, keepdims=True) + 1e-6)
    return (wide * scale * gain).astype(jnp.bfloat16)


def _tables(base, part):
    first = lax.broadcasted_iota(jnp.int32, part.shape, 1) < HEAD // 2
    base = jnp.broadcast_to(base, part.shape)
    base_r, part_r = pltpu.roll(base, HEAD // 2, 1), pltpu.roll(part, HEAD // 2, 1)
    cos_a, sin_a = jnp.where(first, base, base_r), jnp.where(first, base_r, base)
    cos_b, sin_b = jnp.where(first, part, part_r), jnp.where(first, part_r, part)
    cos, sin = cos_a * cos_b - sin_a * sin_b, sin_a * cos_b + cos_a * sin_b
    return cos, jnp.where(first, -sin, sin)


def _turn(t, cos, sin):
    t = t.astype(jnp.bfloat16).astype(jnp.float32)
    return (t * cos + pltpu.roll(t, HEAD // 2, 1) * sin).astype(jnp.bfloat16)


def _kernel(x_ref, gain_ref, wq_ref, wk_ref, wv_ref, wo_ref, base_ref, part_ref, y_ref,
            own, land, wq_s, wk_s, wv_s, q_s, k_s, v_s, a_s, cos_s, sin_s, gap_s, top, mix,
            x_sem, w_sem, pair_send, pair_recv, up_send, link_recv, on_send, side_send, side_recv, o_send, o_recv, free_sem, in_sem, y_sem):
    me = lax.axis_index("sp")
    chip, core = lax.div(me, 2), lax.rem(me, 2)
    pair, up, down = chip * 2 + 1 - core, lax.rem(me + 2, 8), lax.rem(me + 6, 8)
    rows = x_ref.shape[0]
    pieces = rows // PIECE
    steps = chip * pieces
    kv, nq = k_s.shape[0], q_s.shape[1]
    g = q_s.shape[2] // BQ
    cols = g * BQ
    mine = kv * HEAD
    e = HEAD**-0.5 * LOG2E

    def remote(src, dst, send, recv, to):
        return pltpu.make_async_remote_copy(src_ref=src, dst_ref=dst, send_sem=send, recv_sem=recv, device_id={"sp": to},
                                            device_id_type=pl.DeviceIdType.MESH)

    own_copy = pltpu.make_async_copy(x_ref, own.at[core], x_sem)
    own_copy.start()
    kv_tiles, q_tiles = wk_s.shape[0], wq_s.shape[0]

    def kv_copies(n):
        here = pl.ds(pl.multiple_of(core * mine + n * TILE, TILE), TILE)
        return [pltpu.make_async_copy(wk_ref.at[:, here], wk_s.at[n], w_sem.at[2 * n]),
                pltpu.make_async_copy(wv_ref.at[:, here], wv_s.at[n], w_sem.at[2 * n + 1])]

    def q_copy(n):
        here = pl.ds(pl.multiple_of(core * g * mine + n * TILE, TILE), TILE)
        return pltpu.make_async_copy(wq_ref.at[:, here], wq_s.at[n], w_sem.at[2 * kv_tiles + n])

    for n in range(kv_tiles):
        for copy in kv_copies(n):
            copy.start()
    for n in range(q_tiles):
        q_copy(n).start()

    barrier = pltpu.get_barrier_semaphore()
    for other in (pair, up, down):
        pl.semaphore_signal(barrier, inc=1, device_id={"sp": other}, device_id_type=pl.DeviceIdType.MESH)
    pl.semaphore_wait(barrier, 3)

    pair_copy = remote(x_ref, own.at[core], pair_send, pair_recv, pair)
    pair_copy.start()

    def up_copy(n):
        here = pl.ds(n * PIECE, PIECE)
        return remote(x_ref.at[here], land.at[core, n], up_send.at[n], link_recv.at[n], up)

    @pl.when(chip < 3)
    def _():
        for n in range(pieces):
            up_copy(n).start()

    def arrived(t):
        return remote(land.at[core, t], land.at[core, t], on_send.at[t], link_recv.at[t], up)

    def on_copy(t):
        return remote(land.at[core, t], land.at[core, t + pieces], on_send.at[t], link_recv.at[t + pieces], up)

    def side_copy(t):
        return remote(land.at[core, t], land.at[core, t], side_send.at[t], side_recv.at[t], pair)

    def relay(t):
        @pl.when(t < steps)
        def _():
            arrived(t).wait_recv()
            side_copy(t).start()

            @pl.when(chip < 3)
            def _():
                on_copy(t).start()

    gain = gain_ref[...].astype(jnp.float32)[None]

    def turn_own(half):
        cos, sin = _tables(base_ref[pl.ds(chip * 2 + half, 1), :], part_ref[...])
        here = pl.ds(pl.multiple_of(half * rows, rows), rows)
        cos_s[here, :], sin_s[here, :] = cos, sin

    def norm_own(half):
        def some(n, _):
            here = pl.ds(pl.multiple_of(n * PIECE, PIECE), PIECE)
            own[half, here, :] = _normed(own[half, here, :], gain)

        lax.fori_loop(0, pieces, some, None)

    own_copy.wait()
    norm_own(core)
    turn_own(core)
    turn_own(1 - core)
    gap_s[...] = lax.rem(lax.broadcasted_iota(jnp.int32, (BK, cols), 1), BQ) - lax.broadcasted_iota(jnp.int32, (BK, cols), 0)
    top[...] = jnp.full(top.shape, NEG, jnp.float32)
    mix[...] = jnp.zeros(mix.shape, jnp.float32)
    v_s[:, HEAD:, :] = jnp.ones((kv, ONES, v_s.shape[2]), jnp.bfloat16)
    pair_copy.wait_recv()
    norm_own(1 - core)
    per = TILE // HEAD

    def project_kv(n, a, at, size):
        here = pl.ds(at, size)
        cos, sin = cos_s[here, :], sin_s[here, :]
        k = _dot(a, wk_s[n], 1, 0)
        v = _dot(a, wv_s[n], 1, 0)
        for h in range(per):
            part = slice(h * HEAD, (h + 1) * HEAD)
            k_s[n * per + h, here, :] = _turn(k[:, part], cos, sin)
            v_s[n * per + h, :HEAD, here] = v[:, part].astype(jnp.bfloat16).T

    def own_kv(n, _):
        for copy in kv_copies(n):
            copy.wait()
        for half in range(2):
            project_kv(n, own[half], half * rows, rows)

    lax.fori_loop(0, kv_tiles, own_kv, None)

    def own_q(n, _):
        q_copy(n).wait()
        for half in range(2):
            q = _dot(own[half], wq_s[n], 1, 0)
            for b in range(rows // BQ):
                at = half * rows + b * BQ
                cos, sin = cos_s[at : at + BQ, :], sin_s[at : at + BQ, :]
                for h in range(per):
                    head = n * per + h
                    put = pl.ds(pl.multiple_of(lax.rem(head, g) * BQ, BQ), BQ)
                    q_s[lax.div(head, g), half * (rows // BQ) + b, put, :] = _turn(
                        q[b * BQ : (b + 1) * BQ, h * HEAD : (h + 1) * HEAD], cos, sin)

    def own_q_twice(n, _):
        own_q(2 * n, None)
        own_q(2 * n + 1, None)

    lax.fori_loop(0, q_tiles // 2, own_q_twice, None)

    def wo_copy(half, n, to, sem):
        here = pl.ds(pl.multiple_of(half * g * mine, g * mine), g * mine)
        return pltpu.make_async_copy(wo_ref.at[here, pl.ds(n * TILE, TILE)], to, sem)

    wo_mine = [wo_copy(core, n, wq_s.at[n], w_sem.at[2 * kv_tiles + n]) for n in range(q_tiles)]
    wo_other = [wo_copy(1 - core, n, wk_s.at[n], w_sem.at[n]) for n in range(kv_tiles)]
    wo_other += [wo_copy(1 - core, kv_tiles + n, wv_s.at[n], w_sem.at[kv_tiles + n]) for n in range(kv_tiles)]
    for copy in wo_mine:
        copy.start()

    def relays(first, end):
        lax.fori_loop(first, end, lambda t, _: relay(t), None)

    relays(0, 2)

    def block(iq, first, size, masked):
        here = pl.ds(first, size)
        for group in range(0, kv, AT_ONCE):
            heads = range(group, group + AT_ONCE)
            scores = [_dot(k_s[i, here, :], q_s[i, iq], 1, 1) for i in heads]
            if masked:
                ok = gap_s[...] >= first - iq * BQ
            weights, keeps = [], []
            for i, s in zip(heads, scores):
                if masked:
                    s = jnp.where(ok, s, HIDDEN)
                old = top[iq, i : i + 1, :]
                new = jnp.maximum(old, s.max(axis=0, keepdims=True))
                top[iq, i : i + 1, :] = new
                weights.append(jnp.exp2((s - new) * e).astype(jnp.bfloat16))
                keeps.append(jnp.exp2((old - new) * e))
            for i, p, keep in zip(heads, weights, keeps):
                mix[iq, i] = mix[iq, i] * keep + _dot(v_s[i, :, here], p, 1, 0)

    def own_block(iq, _):
        lax.fori_loop(0, iq, lambda j, _: block(iq, pl.multiple_of(j * BK, BK), BK, False), None)
        block(iq, pl.multiple_of(iq * BK, BK), BK, True)

    lax.fori_loop(0, nq, own_block, None)

    def step(t, count, relay_between):
        for n in range(count):
            side_copy(t + n).wait_recv()
        source = chip - 1 - lax.div(t, pieces)
        for half in range(2):
            for n in range(count):
                at = pl.multiple_of(lax.rem(t + n, pieces) * PIECE, PIECE)
                here = slice((half * count + n) * PIECE, (half * count + n + 1) * PIECE)
                a_s[here, :] = _normed(land[half, t + n], gain)
                cos_s[here, :], sin_s[here, :] = _tables(base_ref[pl.ds(source * 2 + half, 1), :], part_ref[pl.ds(at, PIECE), :])
        keys = 2 * count * PIECE

        def some(n, _):
            for m in range(2):
                project_kv(2 * n + m, a_s[:keys, :], 0, keys)

        lax.fori_loop(0, kv_tiles // 2, some, None)
        relay_between()
        lax.fori_loop(0, nq, lambda iq, _: block(iq, 0, keys, False), None)

    def due(u):
        return jnp.where(chip < 3, 2 * u + 4, 2 * u + 2 + jnp.where(u < 2, 1, 0))

    def between(u):
        return due(u) + jnp.where((chip == 3) & ((u == 0) | (u == 2)), 1, 0)

    def double(u, _):
        relays(jnp.where(u == 0, 2, between(u - 1)), due(u))
        step(u * 2, 2, lambda: relays(due(u), between(u)))

    lax.fori_loop(0, chip * (pieces // 2), double, None)

    pl.semaphore_signal(free_sem, inc=1, device_id={"sp": pair}, device_id_type=pl.DeviceIdType.MESH)
    for copy in wo_other:
        copy.start()
    free = 2 * pieces

    @pl.when(chip == 3)
    def _():
        for n in range(pieces):
            side_copy(free + n).wait_send()

    x_copies = [pltpu.make_async_copy(x_ref.at[pl.ds(n * PIECE, PIECE)], land.at[core, free + n], in_sem.at[n]) for n in range(pieces)]
    for copy in x_copies:
        copy.start()

    def finish(half, u):
        iq = half * 2 + u
        for i in range(kv):
            out = mix[iq, i, :HEAD, :] * (1 / mix[iq, i, HEAD : HEAD + 1, :])
            for n in range(g):
                at = (i * g + n) * HEAD
                own[half, u * BQ : (u + 1) * BQ, at : at + HEAD] = out[:, n * BQ : (n + 1) * BQ].T.astype(jnp.bfloat16)

    def o_copy(u):
        here = pl.ds(u * BQ, BQ)
        return remote(own.at[1 - core, here], a_s.at[here], o_send.at[u], o_recv.at[u], pair)

    finish(1 - core, 0)
    pl.semaphore_wait(free_sem, 1)
    finish(1 - core, 1)
    o_copy(0).start()
    finish(core, 0)
    o_copy(1).start()
    finish(core, 1)

    for copy in wo_mine:
        copy.wait()
    blocks = rows // HEAD

    def first_half(n, _):
        y = _dot(own[core], wq_s[n], 1, 0)
        for b in range(blocks):
            slot = lax.rem(2 * n, kv) + b // 2
            mix[lax.div(2 * n, kv), slot, :HEAD, (b % 2) * TILE : (b % 2 + 1) * TILE] = y[b * HEAD : (b + 1) * HEAD]

    lax.fori_loop(0, q_tiles, first_half, None)
    for copy in wo_other + x_copies:
        copy.wait()
    for u in range(2):
        o_copy(u).wait()

    def second_half(base, w_s):
        def some(m, _):
            n = base + m
            here = pl.ds(pl.multiple_of(n * TILE, TILE), TILE)
            y = _dot(a_s[...], w_s[m], 1, 0)
            for b in range(blocks):
                slot = lax.rem(2 * n, kv) + b // 2
                part = mix[lax.div(2 * n, kv), slot, :HEAD, (b % 2) * TILE : (b % 2 + 1) * TILE]
                x = land[core, free + b, :, here].astype(jnp.float32)
                at = slice(b * HEAD, (b + 1) * HEAD)
                own[1 - core, at, here] = (x + (y[at] + part)).astype(jnp.bfloat16)

        lax.fori_loop(0, kv_tiles, some, None)

    def y_copy(n):
        here = pl.ds(n * kv_tiles * TILE, kv_tiles * TILE)
        return pltpu.make_async_copy(own.at[1 - core, :, here], y_ref.at[:, here], y_sem.at[n])

    second_half(0, wk_s)
    y_copy(0).start()
    second_half(kv_tiles, wv_s)
    y_copy(1).start()

    pair_copy.wait_send()

    @pl.when(chip < 3)
    def _():
        for n in range(pieces):
            up_copy(n).wait_send()

    def sent(t, _):
        side_copy(t).wait_send()

        @pl.when(chip < 3)
        def _():
            on_copy(t).wait_send()

    lax.fori_loop(0, jnp.minimum(steps, free), sent, None)
    y_copy(0).wait()
    y_copy(1).wait()


def layer(x, gain, wq, wk, wv, wo, base, part):
    rows, depth = x.shape
    kv = wk.shape[1] // HEAD // 2
    heads = wq.shape[1] // HEAD // 2
    g = heads // kv
    tokens = 2 * rows
    pieces = rows // PIECE
    far = 3 * pieces
    nq = tokens // BQ
    low = jnp.bfloat16
    anywhere = pl.BlockSpec(memory_space=pl.ANY)
    held = pl.BlockSpec(memory_space=pltpu.VMEM)
    dma = pltpu.SemaphoreType.DMA
    return pl.pallas_call(
        _kernel,
        in_specs=[anywhere, held, anywhere, anywhere, anywhere, anywhere, held, held],
        out_specs=anywhere,
        out_shape=jax.ShapeDtypeStruct((rows, depth), low),
        scratch_shapes=[
            pltpu.VMEM((2, rows, depth), low),
            pltpu.VMEM((2, far, PIECE, depth), low),
            pltpu.VMEM((heads * HEAD // TILE, depth, TILE), low),
            pltpu.VMEM((kv * HEAD // TILE, depth, TILE), low),
            pltpu.VMEM((kv * HEAD // TILE, depth, TILE), low),
            pltpu.VMEM((kv, nq, g * BQ, HEAD), low),
            pltpu.VMEM((kv, tokens, HEAD), low),
            pltpu.VMEM((kv, HEAD + ONES, tokens), low),
            pltpu.VMEM((2 * PAIR * PIECE, depth), low),
            pltpu.VMEM((tokens, HEAD), jnp.float32),
            pltpu.VMEM((tokens, HEAD), jnp.float32),
            pltpu.VMEM((BK, g * BQ), jnp.int32),
            pltpu.VMEM((nq, kv, g * BQ), jnp.float32),
            pltpu.VMEM((nq, kv, HEAD + ONES, g * BQ), jnp.float32),
            dma, dma((2 * kv * HEAD // TILE + heads * HEAD // TILE,)), dma, dma,
            dma((pieces,)), dma((far,)), dma((far,)), dma((far,)), dma((far,)),
            dma((2,)), dma((2,)), pltpu.SemaphoreType.REGULAR, dma((pieces,)), dma((2,)),
        ],
        compiler_params=pltpu.CompilerParams(collective_id=0, has_side_effects=True, vmem_limit_bytes=VMEM),
        name="layer",
    )(x, gain, wq, wk, wv, wo, base, part)


def solution(mesh):
    devices = mesh.shape["sp"]

    def step(x, gain, wq, wk, wv, wo):
        rows = x.shape[0]
        base, part = angles(np.arange(devices) * rows), angles(np.arange(rows))
        return layer(x, gain, wq, wk, wv, wo, base, part)

    tokens, whole = P(("dp", "sp"), None), P(None, None)
    return jax.shard_map(
        step,
        mesh=mesh,
        in_specs=(tokens, P(None), whole, whole, whole, whole),
        out_specs=tokens,
        check_vma=False,
    )
```

```python
import functools

import jax
import jax.numpy as jnp
import numpy as np
from jax import lax
from jax.experimental import pallas as pl
from jax.experimental.pallas import tpu as pltpu
from jax.sharding import PartitionSpec as P

HEAD = 128
THETA = 10000
NEG = -1e30
HIDDEN = 2 * NEG
LOG2E = 1.4426950408889634
VMEM = 63 * 2**20
ONES = 8
PIECE = 128
BQ = 256
BK = 256
PAIR = 2
START, STEP = 46, 17
AT_ONCE = 8
TILE = 256


def _dot(a, b, ca, cb):
    return lax.dot_general(a, b, (((ca,), (cb,)), ((), ())), preferred_element_type=jnp.float32)


def angles(place):
    half = HEAD // 2
    angle = place[:, None] * float(THETA) ** (-np.arange(half) / half)
    return jnp.asarray(np.concatenate([np.cos(angle), np.sin(angle)], 1), jnp.float32)


def _normed(x, gain):
    wide = x.astype(jnp.float32)
    scale = lax.rsqrt(jnp.mean(wide * wide, -1, keepdims=True) + 1e-6)
    return (wide * scale * gain).astype(jnp.bfloat16)


def _tables(base, part):
    first = lax.broadcasted_iota(jnp.int32, part.shape, 1) < HEAD // 2
    base = jnp.broadcast_to(base, part.shape)
    base_r, part_r = pltpu.roll(base, HEAD // 2, 1), pltpu.roll(part, HEAD // 2, 1)
    cos_a, sin_a = jnp.where(first, base, base_r), jnp.where(first, base_r, base)
    cos_b, sin_b = jnp.where(first, part, part_r), jnp.where(first, part_r, part)
    cos, sin = cos_a * cos_b - sin_a * sin_b, sin_a * cos_b + cos_a * sin_b
    return cos, jnp.where(first, -sin, sin)


def _turn(t, cos, sin):
    t = t.astype(jnp.bfloat16).astype(jnp.float32)
    return (t * cos + pltpu.roll(t, HEAD // 2, 1) * sin).astype(jnp.bfloat16)


def _kernel(x_ref, gain_ref, wq_ref, wk_ref, wv_ref, wo_ref, base_ref, part_ref, y_ref,
            own, land, wq_s, wk_s, wv_s, q_s, k_s, v_s, a_s, cos_s, sin_s, gap_s, top, mix,
            x_sem, w_sem, pair_send, pair_recv, up_send, link_recv, on_send, side_send, side_recv, o_send, o_recv, free_sem, in_sem, y_sem):
    me = lax.axis_index("sp")
    chip, core = lax.div(me, 2), lax.rem(me, 2)
    pair, up, down = chip * 2 + 1 - core, lax.rem(me + 2, 8), lax.rem(me + 6, 8)
    rows = x_ref.shape[0]
    pieces = rows // PIECE
    steps = chip * pieces
    kv, nq = k_s.shape[0], q_s.shape[1]
    g = q_s.shape[2] // BQ
    cols = g * BQ
    mine = kv * HEAD
    e = HEAD**-0.5 * LOG2E

    def remote(src, dst, send, recv, to):
        return pltpu.make_async_remote_copy(src_ref=src, dst_ref=dst, send_sem=send, recv_sem=recv, device_id={"sp": to},
                                            device_id_type=pl.DeviceIdType.MESH)

    own_copy = pltpu.make_async_copy(x_ref, own.at[core], x_sem)
    own_copy.start()
    kv_tiles, q_tiles = wk_s.shape[0], wq_s.shape[0]

    def kv_copies(n):
        here = pl.ds(pl.multiple_of(core * mine + n * TILE, TILE), TILE)
        return [pltpu.make_async_copy(wk_ref.at[:, here], wk_s.at[n], w_sem.at[2 * n]),
                pltpu.make_async_copy(wv_ref.at[:, here], wv_s.at[n], w_sem.at[2 * n + 1])]

    def q_copy(n):
        here = pl.ds(pl.multiple_of(core * g * mine + n * TILE, TILE), TILE)
        return pltpu.make_async_copy(wq_ref.at[:, here], wq_s.at[n], w_sem.at[2 * kv_tiles + n])

    barrier = pltpu.get_barrier_semaphore()
    for other in (pair, up, down):
        pl.semaphore_signal(barrier, inc=1, device_id={"sp": other}, device_id_type=pl.DeviceIdType.MESH)
    gap_s[...] = lax.rem(lax.broadcasted_iota(jnp.int32, (BK, cols), 1), BQ) - lax.broadcasted_iota(jnp.int32, (BK, cols), 0)
    top[...] = jnp.full(top.shape, NEG, jnp.float32)
    mix[...] = jnp.zeros(mix.shape, jnp.float32)
    v_s[:, HEAD:, :] = jnp.ones((kv, ONES, v_s.shape[2]), jnp.bfloat16)
    pl.semaphore_wait(barrier, 3)

    pair_copy = remote(x_ref, own.at[core], pair_send, pair_recv, pair)
    pair_copy.start()

    def up_copy(n):
        here = pl.ds(n * PIECE, PIECE)
        return remote(x_ref.at[here], land.at[core, n], up_send.at[n], link_recv.at[n], up)

    @pl.when(chip < 3)
    def _():
        for n in range(pieces):
            up_copy(n).start()

    for n in range(kv_tiles):
        for copy in kv_copies(n):
            copy.start()
    for n in range(q_tiles):
        q_copy(n).start()

    def arrived(t):
        return remote(land.at[core, t], land.at[core, t], on_send.at[t], link_recv.at[t], up)

    def on_copy(t):
        return remote(land.at[core, t], land.at[core, t + pieces], on_send.at[t], link_recv.at[t + pieces], up)

    def side_copy(t):
        return remote(land.at[core, t], land.at[core, t], side_send.at[t], side_recv.at[t], pair)

    def relay(t):
        @pl.when(t < steps)
        def _():
            arrived(t).wait_recv()
            side_copy(t).start()

            @pl.when(chip < 3)
            def _():
                on_copy(t).start()

    gain = gain_ref[...].astype(jnp.float32)[None]

    def turn_own(half):
        cos, sin = _tables(base_ref[pl.ds(chip * 2 + half, 1), :], part_ref[...])
        here = pl.ds(pl.multiple_of(half * rows, rows), rows)
        cos_s[here, :], sin_s[here, :] = cos, sin

    def norm_own(half):
        def some(n, _):
            here = pl.ds(pl.multiple_of(n * PIECE, PIECE), PIECE)
            own[half, here, :] = _normed(own[half, here, :], gain)

        lax.fori_loop(0, pieces, some, None)

    own_copy.wait()
    norm_own(core)
    turn_own(core)
    turn_own(1 - core)
    per = TILE // HEAD

    def project_kv(n, a, at, size):
        here = pl.ds(at, size)
        cos, sin = cos_s[here, :], sin_s[here, :]
        k = _dot(a, wk_s[n], 1, 0)
        v = _dot(a, wv_s[n], 1, 0)
        for h in range(per):
            part = slice(h * HEAD, (h + 1) * HEAD)
            k_s[n * per + h, here, :] = _turn(k[:, part], cos, sin)
            v_s[n * per + h, :HEAD, here] = v[:, part].astype(jnp.bfloat16).T

    def project_q(n, half):
        q = _dot(own[half], wq_s[n], 1, 0)
        for b in range(rows // BQ):
            here = pl.ds(pl.multiple_of(half * rows + b * BQ, BQ), BQ)
            cos, sin = cos_s[here, :], sin_s[here, :]
            for h in range(per):
                head = n * per + h
                put = pl.ds(pl.multiple_of(lax.rem(head, g) * BQ, BQ), BQ)
                q_s[lax.div(head, g), half * (rows // BQ) + b, put, :] = _turn(
                    q[b * BQ : (b + 1) * BQ, h * HEAD : (h + 1) * HEAD], cos, sin)

    def own_half(half, first):
        def some_kv(n, _):
            if first:
                for m in range(2):
                    for copy in kv_copies(2 * n + m):
                        copy.wait()
            for m in range(2):
                project_kv(2 * n + m, own[half], pl.multiple_of(half * rows, rows), rows)

        def some_q(n, _):
            if first:
                for m in range(2):
                    q_copy(2 * n + m).wait()
            for m in range(2):
                project_q(2 * n + m, half)

        lax.fori_loop(0, kv_tiles // 2, some_kv, None)
        lax.fori_loop(0, q_tiles // 2, some_q, None)

    own_half(core, True)
    pair_copy.wait_recv()
    norm_own(1 - core)
    own_half(1 - core, False)

    def wo_copy(half, n, to, sem):
        here = pl.ds(pl.multiple_of(half * g * mine, g * mine), g * mine)
        return pltpu.make_async_copy(wo_ref.at[here, pl.ds(n * TILE, TILE)], to, sem)

    wo_mine = [wo_copy(core, n, wq_s.at[n], w_sem.at[2 * kv_tiles + n]) for n in range(q_tiles)]
    wo_other = [wo_copy(1 - core, n, wk_s.at[n], w_sem.at[n]) for n in range(kv_tiles)]
    wo_other += [wo_copy(1 - core, kv_tiles + n, wv_s.at[n], w_sem.at[kv_tiles + n]) for n in range(kv_tiles)]
    for copy in wo_mine:
        copy.start()

    def relays(first, end):
        lax.fori_loop(first, end, lambda t, _: relay(t), None)

    relays(0, 2)

    def block(iq, first, size, masked):
        here = pl.ds(first, size)
        for group in range(0, kv, AT_ONCE):
            heads = range(group, group + AT_ONCE)
            scores = [_dot(k_s[i, here, :], q_s[i, iq], 1, 1) for i in heads]
            if masked:
                ok = gap_s[...] >= first - iq * BQ
            weights, keeps = [], []
            for i, s in zip(heads, scores):
                if masked:
                    s = jnp.where(ok, s, HIDDEN)
                old = top[iq, i : i + 1, :]
                new = jnp.maximum(old, s.max(axis=0, keepdims=True))
                top[iq, i : i + 1, :] = new
                weights.append(jnp.exp2((s - new) * e).astype(jnp.bfloat16))
                keeps.append(jnp.exp2((old - new) * e))
            for i, p, keep in zip(heads, weights, keeps):
                mix[iq, i] = mix[iq, i] * keep + _dot(v_s[i, :, here], p, 1, 0)

    def own_block(iq, _):
        lax.fori_loop(0, iq, lambda j, _: block(iq, pl.multiple_of(j * BK, BK), BK, False), None)
        block(iq, pl.multiple_of(iq * BK, BK), BK, True)

    lax.fori_loop(0, nq, own_block, None)

    def step(t, count, relay_between, relay_late):
        for n in range(count):
            side_copy(t + n).wait_recv()
        source = chip - 1 - lax.div(t, pieces)
        for half in range(2):
            for n in range(count):
                at = pl.multiple_of(lax.rem(t + n, pieces) * PIECE, PIECE)
                here = slice((half * count + n) * PIECE, (half * count + n + 1) * PIECE)
                a_s[here, :] = _normed(land[half, t + n], gain)
                cos_s[here, :], sin_s[here, :] = _tables(base_ref[pl.ds(source * 2 + half, 1), :], part_ref[pl.ds(at, PIECE), :])
        keys = 2 * count * PIECE

        def some(n, _):
            for m in range(2):
                project_kv(2 * n + m, a_s[:keys, :], 0, keys)

        lax.fori_loop(0, kv_tiles // 2, some, None)
        relay_between()
        lax.fori_loop(0, nq // 2, lambda iq, _: block(iq, 0, keys, False), None)
        relay_late()
        lax.fori_loop(nq // 2, nq, lambda iq, _: block(iq, 0, keys, False), None)

    def come(u, after):
        return jnp.minimum(lax.div(4 * (START - 4 + STEP * u + after), 45), steps)

    def due(u, count):
        return jnp.where(chip < 3, 2 * u + 4, jnp.maximum(2 * u + count, come(u, 0)))

    def double(u, done):
        first = due(u, 2)
        relays(done, first)
        then = jnp.where(chip < 3, first, jnp.maximum(first, come(u, 6)))
        late = jnp.where(chip < 3, first, jnp.maximum(first, come(u, 12)))
        step(u * 2, 2, lambda: relays(first, then), lambda: relays(then, late))
        return late

    doubles = chip * (pieces // 2) - jnp.where(chip == 3, 1, 0)
    done = lax.fori_loop(0, doubles, double, 2)

    def single(t, done):
        relays(done, t + 1)
        step(t, 1, lambda: relays(jnp.maximum(done, t + 1), t + 2), lambda: None)
        return t + 2

    lax.fori_loop(doubles * 2, steps, single, done)

    pl.semaphore_signal(free_sem, inc=1, device_id={"sp": pair}, device_id_type=pl.DeviceIdType.MESH)
    for copy in wo_other:
        copy.start()
    free = 2 * pieces

    @pl.when(chip == 3)
    def _():
        for n in range(pieces):
            side_copy(free + n).wait_send()

    x_copies = [pltpu.make_async_copy(x_ref.at[pl.ds(n * PIECE, PIECE)], land.at[core, free + n], in_sem.at[n]) for n in range(pieces)]
    for copy in x_copies:
        copy.start()

    def finish(half, u):
        iq = half * 2 + u
        for i in range(kv):
            out = mix[iq, i, :HEAD, :] * (1 / mix[iq, i, HEAD : HEAD + 1, :])
            for n in range(g):
                at = (i * g + n) * HEAD
                own[half, u * BQ : (u + 1) * BQ, at : at + HEAD] = out[:, n * BQ : (n + 1) * BQ].T.astype(jnp.bfloat16)

    def o_copy(u):
        here = pl.ds(u * BQ, BQ)
        return remote(own.at[1 - core, here], a_s.at[here], o_send.at[u], o_recv.at[u], pair)

    finish(1 - core, 0)
    pl.semaphore_wait(free_sem, 1)
    finish(1 - core, 1)
    o_copy(0).start()
    finish(core, 0)
    o_copy(1).start()
    finish(core, 1)

    for copy in wo_mine:
        copy.wait()
    blocks = rows // HEAD

    def first_half(n, _):
        y = _dot(own[core], wq_s[n], 1, 0)
        for b in range(blocks):
            slot = lax.rem(2 * n, kv) + b // 2
            mix[lax.div(2 * n, kv), slot, :HEAD, (b % 2) * TILE : (b % 2 + 1) * TILE] = y[b * HEAD : (b + 1) * HEAD]

    lax.fori_loop(0, q_tiles, first_half, None)
    for copy in wo_other + x_copies:
        copy.wait()
    for u in range(2):
        o_copy(u).wait()

    def second_half(base, w_s):
        def some(m, _):
            n = base + m
            here = pl.ds(pl.multiple_of(n * TILE, TILE), TILE)
            y = _dot(a_s[...], w_s[m], 1, 0)
            for b in range(blocks):
                slot = lax.rem(2 * n, kv) + b // 2
                part = mix[lax.div(2 * n, kv), slot, :HEAD, (b % 2) * TILE : (b % 2 + 1) * TILE]
                x = land[core, free + b, :, here].astype(jnp.float32)
                at = slice(b * HEAD, (b + 1) * HEAD)
                own[1 - core, at, here] = (x + (y[at] + part)).astype(jnp.bfloat16)

        lax.fori_loop(0, kv_tiles, some, None)

    def y_copy(n):
        here = pl.ds(n * kv_tiles * TILE, kv_tiles * TILE)
        return pltpu.make_async_copy(own.at[1 - core, :, here], y_ref.at[:, here], y_sem.at[n])

    second_half(0, wk_s)
    y_copy(0).start()
    second_half(kv_tiles, wv_s)
    y_copy(1).start()

    pair_copy.wait_send()

    @pl.when(chip < 3)
    def _():
        for n in range(pieces):
            up_copy(n).wait_send()

    def sent(t, _):
        side_copy(t).wait_send()

        @pl.when(chip < 3)
        def _():
            on_copy(t).wait_send()

    lax.fori_loop(0, jnp.minimum(steps, free), sent, None)
    y_copy(0).wait()
    y_copy(1).wait()


def layer(x, gain, wq, wk, wv, wo, base, part):
    rows, depth = x.shape
    kv = wk.shape[1] // HEAD // 2
    heads = wq.shape[1] // HEAD // 2
    g = heads // kv
    tokens = 2 * rows
    pieces = rows // PIECE
    far = 3 * pieces
    nq = tokens // BQ
    low = jnp.bfloat16
    anywhere = pl.BlockSpec(memory_space=pl.ANY)
    held = pl.BlockSpec(memory_space=pltpu.VMEM)
    dma = pltpu.SemaphoreType.DMA
    return pl.pallas_call(
        _kernel,
        in_specs=[anywhere, held, anywhere, anywhere, anywhere, anywhere, held, held],
        out_specs=anywhere,
        out_shape=jax.ShapeDtypeStruct((rows, depth), low),
        scratch_shapes=[
            pltpu.VMEM((2, rows, depth), low),
            pltpu.VMEM((2, far, PIECE, depth), low),
            pltpu.VMEM((heads * HEAD // TILE, depth, TILE), low),
            pltpu.VMEM((kv * HEAD // TILE, depth, TILE), low),
            pltpu.VMEM((kv * HEAD // TILE, depth, TILE), low),
            pltpu.VMEM((kv, nq, g * BQ, HEAD), low),
            pltpu.VMEM((kv, tokens, HEAD), low),
            pltpu.VMEM((kv, HEAD + ONES, tokens), low),
            pltpu.VMEM((2 * PAIR * PIECE, depth), low),
            pltpu.VMEM((tokens, HEAD), jnp.float32),
            pltpu.VMEM((tokens, HEAD), jnp.float32),
            pltpu.VMEM((BK, g * BQ), jnp.int32),
            pltpu.VMEM((nq, kv, g * BQ), jnp.float32),
            pltpu.VMEM((nq, kv, HEAD + ONES, g * BQ), jnp.float32),
            dma, dma((2 * kv * HEAD // TILE + heads * HEAD // TILE,)), dma, dma,
            dma((pieces,)), dma((far,)), dma((far,)), dma((far,)), dma((far,)),
            dma((2,)), dma((2,)), pltpu.SemaphoreType.REGULAR, dma((pieces,)), dma((2,)),
        ],
        compiler_params=pltpu.CompilerParams(collective_id=0, has_side_effects=True, vmem_limit_bytes=VMEM),
        name="layer",
    )(x, gain, wq, wk, wv, wo, base, part)


def solution(mesh):
    devices = mesh.shape["sp"]

    def step(x, gain, wq, wk, wv, wo):
        rows = x.shape[0]
        base, part = angles(np.arange(devices) * rows), angles(np.arange(rows))
        return layer(x, gain, wq, wk, wv, wo, base, part)

    tokens, whole = P(("dp", "sp"), None), P(None, None)
    return jax.shard_map(
        step,
        mesh=mesh,
        in_specs=(tokens, P(None), whole, whole, whole, whole),
        out_specs=tokens,
        check_vma=False,
    )
```
